256 devices in a mesh: ctx: 64 (over z, x, core), tp: 4 (over y).
Axes of the slice: x: 4, y: 4, z: 8, core: 2. Of those that a mesh axis runs over, the one named last changes fastest.
Arguments:
- queries: bfloat16 [8192, 8192], P('ctx', 'tp'), may hold values from -6 to 6
- keys: bfloat16 [32768, 1024], P(('ctx', 'tp')), may hold values from -6 to 6
- values: bfloat16 [32768, 1024], P(('ctx', 'tp')), may hold values from -6 to 6
- grad_out: bfloat16 [8192, 8192], P('ctx', 'tp'), may hold values from -6 to 6
- readers: int32 [64, 4], replicated, may hold values from -1 to 127, as said below
- token_mask: int32 [8192, 4], P('ctx'), may hold values from 0 to 1
- image_len: int32 [128], replicated, may hold values from 64 to 256
Outputs:
- grad_queries: bfloat16 [8192, 8192], P('ctx', 'tp')
- grad_keys: float32 [32768, 1024], P(('ctx', 'tp'))
- grad_values: float32 [32768, 1024], P(('ctx', 'tp'))
The draws below stay inside these ranges and needn't reach their ends.
Inputs may be any that keep to these rules, and one draw needn't show every extreme that they name: `readers`: image m is owned by ctx index m // 2. Row c holds 2 runs of 2 consecutive slots; each run names 2 different images of one owner c - k, the first run with k = 0, the others with different k from 1 to 3; a run whose owner c - k is below 0 is all -1.
All inputs are finite; a program needn't handle non-finite values.
Results may differ from the reference program's by a relative error of at most 0.012.
Values may be sent and summed in bfloat16 or wider, within the bound.
No kernel may reach another device: no remote copies, remote signals or barrier semaphores. Data moves between devices by JAX's collectives and lax.ppermute only.
A program may use at most 64 MiB of HBM per device.

```python
import jax
import jax.numpy as jnp
from jax import lax

HEADS = 64
KVH = 8
HD = 128
TOK_DEV = 128
IMG_DEV = 2
ITOK = 256
SLOTS = 4
CAP = 2
WIN = 4
TOKENS = 8192
IMAGES = 128
N_CTX = 64


def reader_table(key):
    base = jax.random.fold_in(key, 11)
    groups = SLOTS // CAP
    offset_keys = jax.random.split(jax.random.fold_in(base, 1), N_CTX)
    offsets = jax.vmap(lambda subkey: jax.random.permutation(subkey, WIN - 1) + 1)(offset_keys).astype(jnp.int32)
    group_offsets = jnp.concatenate([jnp.zeros((N_CTX, 1), jnp.int32), offsets[:, :groups - 1]], axis=1)
    pick_keys = jax.random.split(jax.random.fold_in(base, 2), N_CTX * groups)
    picks = jax.vmap(lambda subkey: jax.random.permutation(subkey, IMG_DEV)[:CAP])(pick_keys)
    picks = picks.astype(jnp.int32).reshape(N_CTX, groups, CAP)
    owners = jnp.arange(N_CTX, dtype=jnp.int32)[:, None] - group_offsets
    image_ids = owners[:, :, None] * IMG_DEV + picks
    image_ids = jnp.where(owners[:, :, None] >= 0, image_ids, -1)
    return image_ids.reshape(N_CTX, SLOTS).astype(jnp.int32)


def mask_table(key):
    return jax.random.randint(jax.random.fold_in(key, 13), (TOKENS, SLOTS), 0, 2, dtype=jnp.int32)


def key_table(key):
    base = jnp.clip(jax.random.normal(jax.random.fold_in(key, 17), (IMAGES * ITOK, KVH * HD), jnp.float32), -6.0, 6.0)
    return base


def draw_readers(key, part):
    return reader_table(key)


def draw_token_mask(key, part):
    return mask_table(key)


def draw_keys(key, part):
    return key_table(key).astype(jnp.bfloat16)


def draw_queries(key, part):
    base = jnp.clip(jax.random.normal(jax.random.fold_in(key, 19), (TOKENS, HEADS * HD), jnp.float32), -6.0, 6.0)
    return base.astype(jnp.bfloat16)


def plant(result, rng, low, top_value):
    extent = result.shape
    spot = [jax.random.randint(jax.random.fold_in(rng, axis), (), 0, extent[axis]) for axis in range(len(extent))]
    result = result.at[tuple(spot)].set(low)
    longest = extent.index(max(extent))
    spot[longest] = (spot[longest] + 1) % extent[longest]
    return result.at[tuple(spot)].set(top_value)


def levels(key, dims, cuts, least, high):
    def one(dim, parts):
        heights = jax.random.uniform(jax.random.fold_in(jax.random.fold_in(key, 6), dim), (parts,), jnp.float32, least / len(cuts), high / len(cuts))
        return jnp.repeat(jnp.exp(heights), dims[dim] // parts).reshape((-1,) + (1,) * (len(dims) - dim - 1))

    loudness = one(*cuts[0])
    for cut in cuts[1:]:
        loudness = loudness * one(*cut)
    return loudness


def noise(key, shape, deviation, most, cuts=(), kind=jnp.bfloat16):
    factor_of = levels(key, shape, cuts, -0.22, 0.18) if cuts else 1.0
    entries = jax.random.normal(key, shape, jnp.float32) * deviation * factor_of
    return jnp.minimum(jnp.maximum(entries, -most), most).astype(kind)


def setup_inputs(seed: int = 0) -> dict:
    key_list = jax.random.split(jax.random.key(seed), 8)
    queries = draw_queries(jax.random.fold_in(key_list[7], 71), 0)
    keys = draw_keys(jax.random.fold_in(key_list[7], 71), 0)
    values = noise(key_list[2], (IMAGES * ITOK, KVH * HD), 1.0, 6.0, ((0, 256),))
    grad_out = noise(key_list[3], (TOKENS, HEADS * HD), 1.0, 6.0, ((0, 64), (1, 4)))
    readers = draw_readers(jax.random.fold_in(key_list[7], 71), 0)
    token_mask = draw_token_mask(jax.random.fold_in(key_list[7], 71), 0)
    image_len = plant(jax.random.randint(key_list[6], (IMAGES,), ITOK // 4, ITOK + 1), jax.random.fold_in(key_list[6], 1), ITOK // 4, ITOK).astype(jnp.int32)
    return dict(queries=queries, keys=keys, values=values, grad_out=grad_out, readers=readers, token_mask=token_mask, image_len=image_len)


masked_score = -1e+30

def head_grad(query, upstream, key_head, value_head, allowed, scaling):
    scores = jnp.dot(query, key_head.T, preferred_element_type=jnp.float32) * scaling
    scores = jnp.where(allowed, scores, masked_score)
    row_max = lax.optimization_barrier(jnp.max(scores, axis=1, keepdims=True))
    exponent = jnp.where(allowed, jnp.exp(scores - row_max), 0.0)
    totals = jnp.maximum(lax.optimization_barrier(jnp.sum(exponent, axis=1, keepdims=True)), 1.0)
    weights = exponent / totals
    weights_half = weights.astype(jnp.bfloat16)
    attended = jnp.dot(weights_half, value_head, preferred_element_type=jnp.float32)
    row_dot = lax.optimization_barrier(jnp.sum(upstream.astype(jnp.float32) * attended, axis=1, keepdims=True))
    grad_value = jnp.dot(weights_half.T, upstream, preferred_element_type=jnp.float32)
    grad_weights = jnp.dot(upstream, value_head.T, preferred_element_type=jnp.float32)
    scores_half = (weights * (grad_weights - row_dot)).astype(jnp.bfloat16)
    grad_query = jnp.dot(scores_half, key_head, preferred_element_type=jnp.float32) * scaling
    grad_key = jnp.dot(scores_half.T, query, preferred_element_type=jnp.float32) * scaling
    return (grad_query, grad_key, grad_value)

def reference(queries, keys, values, grad_out, readers, token_mask, image_len):
    scaling = HD ** (-0.5)
    per_group = HEADS // KVH
    key_images = keys.reshape(IMAGES, ITOK, KVH, HD)
    value_images = values.reshape(IMAGES, ITOK, KVH, HD)
    positions = jnp.arange(ITOK, dtype=jnp.int32)

    def shard_step(carried, shard):
        grad_keys, grad_values = carried
        image_ids = readers[shard]
        present = image_ids >= 0
        safe_ids = jnp.maximum(image_ids, 0).astype(jnp.int32)
        lengths = image_len[safe_ids]
        start = (shard * TOK_DEV).astype(jnp.int32)
        query_rows = lax.dynamic_slice_in_dim(queries, start, TOK_DEV, 0).reshape(TOK_DEV, HEADS, HD)
        upstream_rows = lax.dynamic_slice_in_dim(grad_out, start, TOK_DEV, 0).reshape(TOK_DEV, HEADS, HD)
        mask_rows = lax.dynamic_slice_in_dim(token_mask, start, TOK_DEV, 0)
        allowed = (mask_rows[:, :, None] == 1) & present[None, :, None] & (positions[None, None, :] < lengths[None, :, None])
        allowed = allowed.reshape(TOK_DEV, SLOTS * ITOK)
        slot_keys = key_images[safe_ids].reshape(SLOTS * ITOK, KVH, HD)
        slot_values = value_images[safe_ids].reshape(SLOTS * ITOK, KVH, HD)
        query_parts = []
        key_parts = []
        value_parts = []
        for head_group in range(KVH):
            key_head = slot_keys[:, head_group]
            value_head = slot_values[:, head_group]

            def head_step(inner, pair):
                grad_query, grad_key, grad_value = head_grad(pair[0], pair[1], key_head, value_head, allowed, scaling)
                return ((inner[0] + grad_key, inner[1] + grad_value), grad_query)
            first = head_group * per_group
            pairs = (jnp.moveaxis(query_rows[:, first:first + per_group], 1, 0), jnp.moveaxis(upstream_rows[:, first:first + per_group], 1, 0))
            zeros = jnp.zeros((SLOTS * ITOK, HD), jnp.float32)
            (group_keys, group_values), group_queries = lax.scan(head_step, (zeros, zeros), pairs)
            query_parts.append(group_queries)
            key_parts.append(group_keys)
            value_parts.append(group_values)
        grad_query = jnp.moveaxis(jnp.concatenate(query_parts, axis=0), 0, 1).reshape(TOK_DEV, HEADS * HD)
        scale_mask = present.astype(jnp.float32)[:, None, None, None]
        slot_grad_keys = jnp.stack(key_parts, axis=1).reshape(SLOTS, ITOK, KVH, HD) * scale_mask
        slot_grad_values = jnp.stack(value_parts, axis=1).reshape(SLOTS, ITOK, KVH, HD) * scale_mask
        grad_keys = grad_keys.at[safe_ids].add(slot_grad_keys)
        grad_values = grad_values.at[safe_ids].add(slot_grad_values)
        return ((grad_keys, grad_values), grad_query.astype(jnp.bfloat16))
    zeros = jnp.zeros((IMAGES, ITOK, KVH, HD), jnp.float32)
    (grad_keys, grad_values), grad_queries = lax.scan(shard_step, (zeros, zeros), jnp.arange(N_CTX, dtype=jnp.int32))
    return (grad_queries.reshape(TOKENS, HEADS * HD), grad_keys.reshape(IMAGES * ITOK, KVH * HD), grad_values.reshape(IMAGES * ITOK, KVH * HD))
```

```python
import jax
import jax.numpy as jnp
from jax import lax
from jax.experimental import pallas as pl
from jax.experimental.pallas import tpu as pltpu
from jax.sharding import PartitionSpec as P

HD = 128
TP = 4
N_CTX = 64
NX = 4
NZ = 8
UNMASKED = 0.0
MASKED = -1e30
ROW_FLOOR = -1e29
LOG2E = 1.4426950408889634
SCALE = HD**-0.5
F32 = jnp.float32
BF16 = jnp.bfloat16

VM = pl.BlockSpec(memory_space=pltpu.VMEM)
SM = pl.BlockSpec(memory_space=pltpu.SMEM)


def route(where):
    pairs = []
    for source in range(N_CTX):
        target = where(source // 2, source % 2)
        if target is not None:
            pairs.append((source, target))
    return pairs


def back(pairs):
    return [(target, source) for source, target in pairs]


def left_of(chip):
    return chip // NX * NX + (chip % NX - 1) % NX


def right_of(chip):
    return chip // NX * NX + (chip % NX + 1) % NX


N_CHIP = N_CTX // 2

SWAP = route(lambda chip, core: chip * 2 + 1 - core)
NEXT = route(lambda chip, core: (chip + 1) * 2 + core if chip + 1 < N_CHIP else None)
FAR_1 = route(lambda chip, core: left_of(chip) * 2 + 1 if core == 1 else chip * 2)
FAR_2 = route(
    lambda chip, core: chip * 2 + 1
    if core == 0
    else ((right_of(chip) + 2) * 2 if right_of(chip) + 2 < N_CHIP else None)
)
FAR_BACK_1 = [(t, s) for s, t in FAR_2 if s % 2 == 1]
FAR_BACK_2 = [(t, s) for s, t in FAR_1 if s % 2 == 1]


def over_ctx(block, pairs):
    return lax.ppermute(block, "ctx", pairs)


def over_tp(block, distance):
    return lax.ppermute(block, "tp", [(i, (i + distance) % TP) for i in range(TP)])


def contract_last(a, b):
    return lax.dot_general(a, b, (((1,), (1,)), ((), ())), preferred_element_type=F32)


def contract(a, b):
    return lax.dot_general(a, b, (((1,), (0,)), ((), ())), preferred_element_type=F32)


def pack_body(place, keys, values, *pieces):
    tp = place[1]
    for d in range(TP):
        start = pl.multiple_of((tp + d) % TP * 256, 256)
        pieces[d][0:128, :] = keys[:, pl.ds(start, 256)]
        pieces[d][128:256, :] = values[:, pl.ds(start, 256)]


def pack(place, keys, values):
    return pl.pallas_call(
        pack_body,
        in_specs=[SM, VM, VM],
        out_specs=[VM] * TP,
        out_shape=[jax.ShapeDtypeStruct((256, 256), BF16)] * TP,
        compiler_params=pltpu.CompilerParams(vmem_limit_bytes=8 * 2**20),
        name="pack",
    )(place, keys, values)


def unpack_body(place, *refs):
    pieces, grad_keys, grad_values = refs[:TP], refs[TP], refs[TP + 1]
    tp = place[1]
    for d in range(TP):
        start = pl.multiple_of((tp + d) % TP * 256, 256)
        grad_keys[:, pl.ds(start, 256)] = pieces[d][0:128, :].astype(F32)
        grad_values[:, pl.ds(start, 256)] = pieces[d][128:256, :].astype(F32)


def unpack(place, pieces):
    return pl.pallas_call(
        unpack_body,
        in_specs=[SM] + [VM] * TP,
        out_specs=[VM] * 2,
        out_shape=[jax.ShapeDtypeStruct((128, 1024), F32)] * 2,
        compiler_params=pltpu.CompilerParams(vmem_limit_bytes=8 * 2**20),
        name="unpack",
    )(place, *pieces)


def attend_body(
    place, readers, image_len, queries, grad_out, token_mask, own, near, swapped, far,
    grad_queries, grad_own, grad_far,
    key_rows, value_rows, bias, weights, score_grads, query_cols, upstream_cols,
):
    ctx = place[0]
    tp = place[1]
    core = ctx % 2
    first_own = readers[ctx, 0]
    first_far = readers[ctx, 2]
    present = first_far >= 0
    owner = jnp.maximum(first_far, 0) // 2
    offset = jnp.where(present, ctx - owner, 2)
    use_near = offset == 2
    use_swapped = jnp.where(core == 0, offset == 1, offset == 3)

    def fill(source, base):
        for d in range(TP):
            for g in range(2):
                rows = slice(base + d * 128, base + (d + 1) * 128)
                cols = slice(g * 128, (g + 1) * 128)
                key_rows[g, rows, :] = source[d * 256 : d * 256 + 128, cols]
                value_rows[g, rows, :] = source[d * 256 + 128 : d * 256 + 256, cols]

    fill(own, 0)

    @pl.when(use_near)
    def _():
        fill(near, 512)

    @pl.when(use_swapped)
    def _():
        fill(swapped, 512)

    @pl.when(jnp.logical_not(use_near | use_swapped))
    def _():
        fill(far, 512)

    lane = lax.broadcasted_iota(jnp.int32, (128, 128), 1)
    marks = token_mask[...]
    for half in range(2):
        base = (ctx if half == 0 else owner) * 2
        first = first_own if half == 0 else first_far
        mark_a = marks[:, 2 * half : 2 * half + 1]
        mark_b = marks[:, 2 * half + 1 : 2 * half + 2]
        for d in range(TP):
            source = (tp + TP - d) % TP
            image = base + source // 2
            mark = jnp.where(first == image, mark_a, mark_b)
            length = image_len[image]
            if half == 1:
                length = jnp.where(present, length, 0)
            allowed = (mark == 1) & (lane + source % 2 * 128 < length)
            cols = slice(half * 512 + d * 128, half * 512 + (d + 1) * 128)
            bias[:, cols] = jnp.where(allowed, UNMASKED, MASKED)

    for g in range(2):

        def head_pair(j, _):
            head = g * 8 + 2 * j
            left = pl.multiple_of(head * 128, 128)
            right = pl.multiple_of(head * 128 + 128, 128)
            query = jnp.concatenate([queries[:, pl.ds(left, 128)], queries[:, pl.ds(right, 128)]], 0)
            upstream = jnp.concatenate([grad_out[:, pl.ds(left, 128)], grad_out[:, pl.ds(right, 128)]], 0)
            pair_bias = jnp.concatenate([bias[...], bias[...]], 0)
            scores = contract_last(query, key_rows[g]) * (SCALE * LOG2E) + pair_bias
            row_max = jnp.maximum(jnp.max(scores, axis=1, keepdims=True), ROW_FLOOR)
            exponent = jnp.exp2(scores - row_max)
            inverse = 1.0 / jnp.maximum(jnp.sum(exponent, axis=1, keepdims=True), 1.0)
            grad_weights = contract_last(upstream, value_rows[g])
            row_dot = jnp.sum(exponent * grad_weights, axis=1, keepdims=True) * inverse
            row = pl.multiple_of(j * 256, 256)
            score_grad = (exponent * (grad_weights - row_dot)).astype(BF16)
            weights[pl.ds(row, 256), :] = exponent.astype(BF16)
            score_grads[pl.ds(row, 256), :] = score_grad
            grad_query = contract(score_grad, key_rows[g]) * (inverse * SCALE)
            grad_queries[:, pl.ds(left, 128)] = grad_query[:128].astype(BF16)
            grad_queries[:, pl.ds(right, 128)] = grad_query[128:].astype(BF16)
            query_cols[:, pl.ds(row, 256)] = (query.astype(F32) * inverse).T.astype(BF16)
            upstream_cols[:, pl.ds(row, 256)] = (upstream.astype(F32) * inverse).T.astype(BF16)
            return 0

        lax.fori_loop(0, 4, head_pair, 0, unroll=True)
        grad_key = (contract(query_cols[...], score_grads[...]) * SCALE).T
        grad_value = contract(upstream_cols[...], weights[...]).T
        cols = slice(g * 128, (g + 1) * 128)
        for d in range(TP):
            keys_at = slice(d * 256, d * 256 + 128)
            values_at = slice(d * 256 + 128, d * 256 + 256)
            own_rows = slice(d * 128, (d + 1) * 128)
            far_rows = slice(512 + d * 128, 512 + (d + 1) * 128)
            grad_own[keys_at, cols] = grad_key[own_rows]
            grad_own[values_at, cols] = grad_value[own_rows]
            grad_far[keys_at, cols] = grad_key[far_rows].astype(BF16)
            grad_far[values_at, cols] = grad_value[far_rows].astype(BF16)


def attend(place, readers, image_len, queries, grad_out, token_mask, own, near, swapped, far):
    return pl.pallas_call(
        attend_body,
        in_specs=[SM] * 3 + [VM] * 7,
        out_specs=[VM] * 3,
        out_shape=[
            jax.ShapeDtypeStruct((128, 2048), BF16),
            jax.ShapeDtypeStruct((1024, 256), F32),
            jax.ShapeDtypeStruct((1024, 256), BF16),
        ],
        scratch_shapes=[
            pltpu.VMEM((2, 1024, 128), BF16),
            pltpu.VMEM((2, 1024, 128), BF16),
            pltpu.VMEM((128, 1024), F32),
            pltpu.VMEM((1024, 1024), BF16),
            pltpu.VMEM((1024, 1024), BF16),
            pltpu.VMEM((128, 1024), BF16),
            pltpu.VMEM((128, 1024), BF16),
        ],
        compiler_params=pltpu.CompilerParams(vmem_limit_bytes=16 * 2**20),
        name="attend",
    )(place, readers, image_len, queries, grad_out, token_mask, own, near, swapped, far)


def offset_of(readers, ctx):
    first = jnp.where(ctx < N_CTX, readers[jnp.minimum(ctx, N_CTX - 1), 2], -1)
    return jnp.where(first >= 0, ctx - first // 2, 0)


def on_device(queries, keys, values, grad_out, readers, token_mask, image_len):
    ctx = lax.axis_index("ctx")
    tp = lax.axis_index("tp")
    core = ctx % 2
    place = jnp.stack([ctx, tp]).astype(jnp.int32)
    pieces = pack(place, keys, values)
    own = jnp.concatenate([pieces[0]] + [over_tp(pieces[d], d) for d in range(1, TP)], 0)
    near = over_ctx(own, NEXT)
    far = over_ctx(over_ctx(own, FAR_1), FAR_2)
    swapped = over_ctx(near, SWAP)
    grad_queries, grad_own, grad_far = attend(
        place, readers, image_len, queries, grad_out, token_mask, own, near, swapped, far
    )
    mine = offset_of(readers, ctx)
    partner = offset_of(readers, ctx + 1 - 2 * core)
    two_on = offset_of(readers, ctx + 3)
    grad_partner = over_ctx(grad_far, SWAP)
    grad_two_on = over_ctx(over_ctx(grad_far, FAR_BACK_1), FAR_BACK_2)
    send_partner = jnp.where(core == 0, partner == 3, partner == 1)
    sent = jnp.where(mine == 2, grad_far, 0).astype(F32) + jnp.where(send_partner, grad_partner, 0).astype(F32)
    grad_next = over_ctx(sent.astype(BF16), back(NEXT))
    total = (
        grad_own
        + grad_next.astype(F32)
        + jnp.where((core == 0) & (partner == 1), grad_partner, 0).astype(F32)
        + jnp.where((core == 1) & (two_on == 3), grad_two_on, 0).astype(F32)
    ).astype(BF16)
    parts = [total[d * 256 : (d + 1) * 256] for d in range(TP)]
    grad_keys, grad_values = unpack(place, [parts[0]] + [over_tp(parts[d], -d) for d in range(1, TP)])
    return (grad_queries, grad_keys, grad_values)


def solution(mesh):
    return jax.shard_map(
        on_device,
        mesh=mesh,
        in_specs=(
            P("ctx", "tp"),
            P(("ctx", "tp"), None),
            P(("ctx", "tp"), None),
            P("ctx", "tp"),
            P(),
            P("ctx", None),
            P(),
        ),
        out_specs=(P("ctx", "tp"), P(("ctx", "tp"), None), P(("ctx", "tp"), None)),
        check_vma=False,
    )
```

```python
import functools

import jax
import jax.numpy as jnp
from jax import lax
from jax.experimental import pallas as pl
from jax.experimental.pallas import tpu as pltpu
from jax.sharding import PartitionSpec as P


HD = 128
TP = 4
N_CTX = 64
UNMASKED = 0.0
MASKED = -1e30
ROW_FLOOR = -1e29
LOG2E = 1.4426950408889634
SCALE = HD**-0.5
F32 = jnp.float32
BF16 = jnp.bfloat16

VM = pl.BlockSpec(memory_space=pltpu.VMEM)
SM = pl.BlockSpec(memory_space=pltpu.SMEM)
ANY = pl.BlockSpec(memory_space=pl.ANY)
HBM = pl.BlockSpec(memory_space=pltpu.HBM)


def route(where):
    pairs = []
    for source in range(N_CTX):
        target = where(source // 2, source % 2)
        if target is not None:
            pairs.append((source, target))
    return pairs


def back(pairs):
    return [(target, source) for source, target in pairs]


N_CHIP = N_CTX // 2

SWAP = route(lambda chip, core: chip * 2 + 1 - core)
NEXT = route(lambda chip, core: (chip + 1) % N_CHIP * 2 + core)
ONWARD = route(lambda chip, core: (chip * 2 + core + 1) % N_CTX)
ONWARD_BACK = back(ONWARD)


def over_ctx(block, pairs):
    return lax.ppermute(block, "ctx", pairs)


def over_tp(block, distance):
    return lax.ppermute(block, "tp", [(i, (i + distance) % TP) for i in range(TP)])


def contract_last(a, b):
    return lax.dot_general(a, b, (((1,), (1,)), ((), ())), preferred_element_type=F32)


def contract(a, b):
    return lax.dot_general(a, b, (((1,), (0,)), ((), ())), preferred_element_type=F32)


def combine_body(flags, grad_far, grad_partner, grad_onward, sent):
    total = jnp.where(flags[1] == 1, grad_far[...], 0).astype(F32)
    total = total + jnp.where(flags[2] == 1, grad_partner[...], 0).astype(F32)
    total = total + jnp.where(flags[3] == 1, grad_onward[...], 0).astype(F32)
    sent[...] = total.astype(BF16)


def combine(flags, *grads):
    return pl.pallas_call(
        combine_body,
        in_specs=[SM] + [VM] * 3,
        out_specs=VM,
        out_shape=jax.ShapeDtypeStruct((512, 256), BF16),
        compiler_params=pltpu.CompilerParams(vmem_limit_bytes=2 * 2**20),
        name="combine",
    )(flags, *grads)


def gather_body(base, flags, grad_own, grad_next, grad_partner, *pieces):
    for d in range(2):
        rows = slice(d * 256, (d + 1) * 256)
        total = grad_own[base + d * 256 : base + (d + 1) * 256, :] + grad_next[rows, :].astype(F32)
        total = total + jnp.where(flags[4] == 1, grad_partner[rows, :], 0).astype(F32)
        pieces[d][...] = total.astype(BF16)


def gather(flags, base, *grads):
    return pl.pallas_call(
        functools.partial(gather_body, base),
        in_specs=[SM] + [VM] * 3,
        out_specs=[VM] * 2,
        out_shape=[jax.ShapeDtypeStruct((256, 256), BF16)] * 2,
        compiler_params=pltpu.CompilerParams(vmem_limit_bytes=2 * 2**20),
        name="gather",
    )(flags, *grads)


def unpack_body(place, *refs):
    pieces, grad_keys, grad_values = refs[:TP], refs[TP], refs[TP + 1]
    tp = place[1]
    for d in range(TP):
        start = pl.multiple_of((tp + d) % TP * 256, 256)
        grad_keys[:, pl.ds(start, 256)] = pieces[d][0:128, :].astype(F32)
        grad_values[:, pl.ds(start, 256)] = pieces[d][128:256, :].astype(F32)


def unpack(place, pieces):
    return pl.pallas_call(
        unpack_body,
        in_specs=[SM] + [VM] * TP,
        out_specs=[VM] * 2,
        out_shape=[jax.ShapeDtypeStruct((128, 1024), F32)] * 2,
        compiler_params=pltpu.CompilerParams(vmem_limit_bytes=4 * 2**20),
        name="unpack",
    )(place, *pieces)


def shaped(shape, dtype):
    return jax.ShapeDtypeStruct(shape, dtype)


def back_of(readers, reader):
    first = readers[2, jnp.minimum(reader, N_CTX - 1)]
    return jnp.where((reader < N_CTX) & (first >= 0), reader - jnp.maximum(first, 0) // 2, 0)


def marks_of(token_mask, slot):
    return [jnp.broadcast_to(token_mask[slot + i : slot + i + 1, :].astype(F32), (128, 128)).T for i in range(2)]


def fill_bias(bias, tp, owner, first, present, marks, image_len):
    lane = lax.broadcasted_iota(jnp.int32, (128, 128), 1)
    for d in range(TP):
        source = (tp + TP - d) % TP
        image = owner * 2 + source // 2
        mark = jnp.where(first == image, marks[0], marks[1])
        length = jnp.where(present, image_len[image], 0)
        allowed = (mark > 0.5) & (lane + source % 2 * 128 < length)
        bias[:, d * 128 : (d + 1) * 128] = jnp.where(allowed, UNMASKED, MASKED)


def plan_body(
    place, readers, image_len, token_mask, queries_hbm, grad_out_hbm,
    flags, own_bias, far_bias, queries, grad_out,
    arrived,
):
    copies = [
        pltpu.make_async_copy(queries_hbm, queries, arrived.at[0]),
        pltpu.make_async_copy(grad_out_hbm, grad_out, arrived.at[1]),
    ]
    for copy in copies:
        copy.start()
    ctx = place[0]
    core = ctx % 2
    first_far = readers[2, ctx]
    owner = jnp.maximum(first_far, 0) // 2
    mine = back_of(readers, ctx)
    partner = back_of(readers, ctx + 1 - 2 * core)
    onward = back_of(readers, ctx + 1)
    swapped = jnp.where(core == 0, mine == 1, mine == 3)
    near = (mine == 2) | (first_far < 0)
    flags[0] = jnp.where(near, 0, jnp.where(swapped, 1, 2))
    flags[1] = (mine == 2).astype(jnp.int32)
    flags[2] = jnp.where(core == 0, partner == 3, partner == 1).astype(jnp.int32)
    flags[3] = ((core == 1) & (onward == 3)).astype(jnp.int32)
    flags[4] = ((core == 0) & (partner == 1)).astype(jnp.int32)
    fill_bias(own_bias, place[1], ctx, readers[0, ctx], True, marks_of(token_mask, 0), image_len)
    fill_bias(far_bias, place[1], owner, first_far, first_far >= 0, marks_of(token_mask, 2), image_len)
    for copy in copies:
        copy.wait()


def plan(place, readers, image_len, token_mask, queries, grad_out):
    return pl.pallas_call(
        plan_body,
        in_specs=[SM] * 3 + [VM] + [HBM] * 2,
        out_specs=[SM] + [VM] * 4,
        out_shape=[
            shaped((8,), jnp.int32),
            shaped((128, 512), F32),
            shaped((128, 512), F32),
            shaped((128, 2048), BF16),
            shaped((128, 2048), BF16),
        ],
        scratch_shapes=[pltpu.SemaphoreType.DMA((2,))],
        compiler_params=pltpu.CompilerParams(vmem_limit_bytes=6 * 2**20),
        cost_estimate=pl.CostEstimate(flops=100000000, bytes_accessed=4194304, transcendentals=0),
        name="plan",
    )(place, readers, image_len, token_mask, queries, grad_out)


def split_rows(halves, key_rows, value_rows):
    for d in range(TP):
        source, base = halves[d // 2], d % 2 * 256
        for g in range(2):
            rows = slice(d * 128, (d + 1) * 128)
            cols = slice(g * 128, (g + 1) * 128)
            key_rows[g, rows, :] = source[base : base + 128, cols]
            value_rows[g, rows, :] = source[base + 128 : base + 256, cols]


def two_heads(ref, head):
    left = pl.multiple_of(head * 128, 128)
    right = pl.multiple_of(head * 128 + 128, 128)
    return jnp.concatenate([ref[:, pl.ds(left, 128)], ref[:, pl.ds(right, 128)]], 0)


def across(column):
    return jnp.broadcast_to(column, (256, 128))


def half_scores(query, upstream, keys, values, bias):
    pair_bias = jnp.concatenate([bias, bias], 0)
    scores = contract_last(query, keys) * (SCALE * LOG2E) + pair_bias
    row_max = jnp.maximum(jnp.max(scores, axis=1, keepdims=True), ROW_FLOOR)
    exponent = jnp.exp2(scores - row_max)
    total = jnp.sum(exponent, axis=1, keepdims=True)
    grad_weights = contract_last(upstream, values)
    dot = jnp.sum(exponent * grad_weights, axis=1, keepdims=True)
    return exponent, grad_weights, row_max, total, dot


def store_grads(halves, g, grad_key, grad_value):
    cols = slice(g * 128, (g + 1) * 128)
    for d in range(TP):
        target, base = halves[d // 2], d % 2 * 256
        rows = slice(d * 128, (d + 1) * 128)
        target[base : base + 128, cols] = grad_key[rows].astype(target.dtype)
        target[base + 128 : base + 256, cols] = grad_value[rows].astype(target.dtype)


def own_body(
    queries, grad_out, bias, own_lo, own_hi,
    exponents, grad_weights, stats,
    key_rows, value_rows,
):
    split_rows((own_lo, own_hi), key_rows, value_rows)
    for g in range(2):

        def head_pair(j, _):
            head = g * 8 + 2 * j
            exponent, weight_grads, row_max, total, dot = half_scores(
                two_heads(queries, head), two_heads(grad_out, head), key_rows[g], value_rows[g], bias[...]
            )
            rows = pl.ds(pl.multiple_of(head * 128, 256), 256)
            exponents[rows, :] = exponent.astype(BF16)
            grad_weights[rows, :] = weight_grads
            stats[rows, 0:128] = across(row_max)
            stats[rows, 128:256] = across(total)
            stats[rows, 256:384] = across(dot)
            return 0

        lax.fori_loop(0, 4, head_pair, 0, unroll=True)


def far_body(
    flags, queries, grad_out, bias, stats,
    near_lo, near_hi, swapped_lo, swapped_hi, onward_lo, onward_hi,
    grad_lo, grad_hi, score_grads, far_keys, factors,
    chosen, value_rows, exponents, query_cols, upstream_cols, arrived,
):
    use_near = flags[0] == 0
    use_swapped = flags[0] == 1

    def fetch(lo, hi):
        return [
            pltpu.make_async_copy(lo, chosen.at[0], arrived.at[0]),
            pltpu.make_async_copy(hi, chosen.at[1], arrived.at[1]),
        ]

    @pl.when(use_near)
    def _():
        for copy in fetch(near_lo, near_hi):
            copy.start()

    @pl.when(use_swapped)
    def _():
        for copy in fetch(swapped_lo, swapped_hi):
            copy.start()

    @pl.when(jnp.logical_not(use_near | use_swapped))
    def _():
        for copy in fetch(onward_lo, onward_hi):
            copy.start()

    for copy in fetch(near_lo, near_hi):
        copy.wait()
    split_rows((chosen.at[0], chosen.at[1]), far_keys, value_rows)
    for g in range(2):

        def head_pair(j, _):
            head = g * 8 + 2 * j
            query, upstream = two_heads(queries, head), two_heads(grad_out, head)
            exponent, weight_grads, far_max, far_total, far_dot = half_scores(
                query, upstream, far_keys[g], value_rows[g], bias[...]
            )
            rows = pl.ds(pl.multiple_of(head * 128, 256), 256)
            own_max = stats[rows, 0:128]
            far_max = across(far_max)
            row_max = jnp.maximum(own_max, far_max)
            own_factor = jnp.exp2(own_max - row_max)
            far_factor = jnp.exp2(far_max - row_max)
            total = stats[rows, 128:256] * own_factor + across(far_total) * far_factor
            inverse = 1.0 / jnp.maximum(total, 1.0)
            own_factor = own_factor * inverse
            far_factor = far_factor * inverse
            row_dot = stats[rows, 256:384] * own_factor + across(far_dot) * far_factor
            factors[rows, 0:128] = own_factor
            factors[rows, 128:256] = far_factor
            factors[rows, 256:384] = row_dot
            row_dot = jnp.concatenate([row_dot] * 4, 1)
            here = pl.ds(pl.multiple_of(j * 256, 256), 256)
            score_grads[rows, :] = (exponent * (weight_grads - row_dot)).astype(BF16)
            exponents[here, :] = exponent.astype(BF16)
            query_cols[:, here] = (query.astype(F32) * far_factor).T.astype(BF16)
            upstream_cols[:, here] = (upstream.astype(F32) * far_factor).T.astype(BF16)
            return 0

        lax.fori_loop(0, 4, head_pair, 0, unroll=True)
        grad_key = (contract(query_cols[...], score_grads[g * 1024 : (g + 1) * 1024, :]) * SCALE).T
        grad_value = contract(upstream_cols[...], exponents[...]).T
        store_grads((grad_lo, grad_hi), g, grad_key, grad_value)


def rest_body(
    queries, grad_out, own_lo, own_hi, exponents, grad_weights, far_score_grads, far_keys, factors,
    grad_queries, grad_own,
    key_rows, value_rows, score_grads, query_cols, upstream_cols,
):
    split_rows((own_lo, own_hi), key_rows, value_rows)
    for g in range(2):

        def head_pair(j, _):
            head = g * 8 + 2 * j
            rows = pl.ds(pl.multiple_of(head * 128, 256), 256)
            own_factor = factors[rows, 0:128]
            far_factor = factors[rows, 128:256]
            row_dot = jnp.concatenate([factors[rows, 256:384]] * 4, 1)
            score_grad = (exponents[rows, :].astype(F32) * (grad_weights[rows, :] - row_dot)).astype(BF16)
            here = pl.ds(pl.multiple_of(j * 256, 256), 256)
            score_grads[here, :] = score_grad
            grad_query = (
                contract(score_grad, key_rows[g]) * own_factor
                + contract(far_score_grads[rows, :], far_keys[g]) * far_factor
            ) * SCALE
            left = pl.multiple_of(head * 128, 128)
            right = pl.multiple_of(head * 128 + 128, 128)
            grad_queries[:, pl.ds(left, 128)] = grad_query[:128].astype(BF16)
            grad_queries[:, pl.ds(right, 128)] = grad_query[128:].astype(BF16)
            query_cols[:, here] = (two_heads(queries, head).astype(F32) * own_factor).T.astype(BF16)
            upstream_cols[:, here] = (two_heads(grad_out, head).astype(F32) * own_factor).T.astype(BF16)
            return 0

        lax.fori_loop(0, 4, head_pair, 0, unroll=True)
        grad_key = (contract(query_cols[...], score_grads[...]) * SCALE).T
        grad_value = contract(upstream_cols[...], exponents[g * 1024 : (g + 1) * 1024, :]).T
        store_grads((grad_own.at[0:512, :], grad_own.at[512:1024, :]), g, grad_key, grad_value)


def own_phase(queries, grad_out, bias, own_lo, own_hi):
    return pl.pallas_call(
        own_body,
        in_specs=[VM] * 5,
        out_specs=[VM] * 3,
        out_shape=[shaped((2048, 512), BF16), shaped((2048, 512), F32), shaped((2048, 384), F32)],
        scratch_shapes=[pltpu.VMEM((2, 512, 128), BF16), pltpu.VMEM((2, 512, 128), BF16)],
        compiler_params=pltpu.CompilerParams(vmem_limit_bytes=12 * 2**20),
        cost_estimate=pl.CostEstimate(flops=600000000, bytes_accessed=4194304, transcendentals=1048576),
        name="own_phase",
    )(queries, grad_out, bias, own_lo, own_hi)


def far_phase(flags, queries, grad_out, bias, stats, *blocks):
    return pl.pallas_call(
        far_body,
        in_specs=[SM] + [VM] * 4 + [ANY] * 6,
        out_specs=[VM] * 5,
        out_shape=[
            shaped((512, 256), BF16),
            shaped((512, 256), BF16),
            shaped((2048, 512), BF16),
            shaped((2, 512, 128), BF16),
            shaped((2048, 384), F32),
        ],
        scratch_shapes=[
            pltpu.VMEM((2, 512, 256), BF16),
            pltpu.VMEM((2, 512, 128), BF16),
            pltpu.VMEM((1024, 512), BF16),
            pltpu.VMEM((128, 1024), BF16),
            pltpu.VMEM((128, 1024), BF16),
            pltpu.SemaphoreType.DMA((2,)),
        ],
        compiler_params=pltpu.CompilerParams(vmem_limit_bytes=12 * 2**20),
        cost_estimate=pl.CostEstimate(flops=1100000000, bytes_accessed=4194304, transcendentals=1048576),
        name="far_phase",
    )(flags, queries, grad_out, bias, stats, *blocks)


def rest_phase(queries, grad_out, own_lo, own_hi, exponents, grad_weights, far_score_grads, far_keys, factors):
    return pl.pallas_call(
        rest_body,
        in_specs=[VM] * 9,
        out_specs=[VM] * 2,
        out_shape=[shaped((128, 2048), BF16), shaped((1024, 256), F32)],
        scratch_shapes=[
            pltpu.VMEM((2, 512, 128), BF16),
            pltpu.VMEM((2, 512, 128), BF16),
            pltpu.VMEM((1024, 512), BF16),
            pltpu.VMEM((128, 1024), BF16),
            pltpu.VMEM((128, 1024), BF16),
        ],
        compiler_params=pltpu.CompilerParams(vmem_limit_bytes=12 * 2**20),
        cost_estimate=pl.CostEstimate(flops=1100000000, bytes_accessed=4194304, transcendentals=1048576),
        name="rest_phase",
    )(queries, grad_out, own_lo, own_hi, exponents, grad_weights, far_score_grads, far_keys, factors)


def on_device(queries, keys, values, grad_out, readers, token_mask, image_len):
    place = jnp.stack([lax.axis_index("ctx"), lax.axis_index("tp")]).astype(jnp.int32)
    core = lax.axis_index("ctx") % 2
    tp = lax.axis_index("tp")
    starts = [(tp + d) % TP * 256 for d in range(TP)]
    pieces = [
        jnp.concatenate([lax.dynamic_slice(x, (0, start), (128, 256)) for x in (keys, values)], 0) for start in starts
    ]
    flags, own_bias, far_bias, queries, grad_out = plan(place, readers.T, image_len, token_mask.T, queries, grad_out)
    own_lo = jnp.concatenate([pieces[0], over_tp(pieces[1], 1)], 0)
    own_hi = jnp.concatenate([over_tp(pieces[2], 2), over_tp(pieces[3], 3)], 0)

    def fetch(own):
        near = over_ctx(own, NEXT)
        sent = jnp.where(core == 1, near, own)
        return near, over_ctx(near, SWAP), over_ctx(sent, ONWARD)

    lo, hi = fetch(own_lo), fetch(own_hi)
    exponents, grad_weights, stats = own_phase(queries, grad_out, own_bias, own_lo, own_hi)
    blocks = [half[i] for i in range(3) for half in (lo, hi)]
    grad_lo, grad_hi, score_grads, far_keys, factors = far_phase(
        flags, queries, grad_out, far_bias, stats, *blocks
    )

    def give(grad):
        onward = over_ctx(grad, ONWARD_BACK)
        partner = over_ctx(grad, SWAP)
        sent = combine(flags, grad, partner, onward)
        return over_ctx(sent, back(NEXT)), partner

    next_hi, partner_hi = give(grad_hi)
    next_lo, partner_lo = give(grad_lo)
    grad_queries, grad_own = rest_phase(
        queries, grad_out, own_lo, own_hi, exponents, grad_weights, score_grads, far_keys, factors
    )
    part_2, part_3 = gather(flags, 512, grad_own, next_hi, partner_hi)
    part_0, part_1 = gather(flags, 0, grad_own, next_lo, partner_lo)
    parts = [part_0, over_tp(part_1, -1), over_tp(part_2, -2), over_tp(part_3, -3)]
    grad_keys, grad_values = unpack(place, parts)
    return (grad_queries, grad_keys, grad_values)


def solution(mesh):
    return jax.shard_map(
        on_device,
        mesh=mesh,
        in_specs=(
            P("ctx", "tp"),
            P(("ctx", "tp"), None),
            P(("ctx", "tp"), None),
            P("ctx", "tp"),
            P(),
            P("ctx", None),
            P(),
        ),
        out_specs=(P("ctx", "tp"), P(("ctx", "tp"), None), P(("ctx", "tp"), None)),
        check_vma=False,
    )
```
